32 devices in a mesh: seq: 8 (over y, x, core), exp: 4 (over z).
Axes of the slice: x: 2, y: 2, z: 4, core: 2. Of those that a mesh axis runs over, the one named last changes fastest.
Arguments:
- grad_out: bfloat16 [4096, 2048], P(('seq', 'exp')), may hold values from -6 to 6
- out_proj: bfloat16 [4096, 2048], P('exp'), may hold values from -0.125 to 0.125
- step_size: float32 [64, 4096], P('exp', 'seq'), may hold values from 0.001 to 0.1
- log_decay: float32 [64, 4096], P('exp', 'seq'), may hold values from -1 to 0, as said below
- b_input: float32 [16, 4096], P(None, 'seq'), may hold values from -1.5 to 1.5
- c_output: float32 [16, 4096], P(None, 'seq'), may hold values from -1.5 to 1.5
- skip_gain: float32 [4096], P('exp'), may hold values from 0.5 to 1.5
- expert_ids: int32 [4096, 2], P('seq'), may hold values from 0 to 3, all different within a row; in each aligned block of 128 rows (0 to 127, 128 to 255, ...) at most 66 rows name the same one
- hidden_act: bfloat16 [4, 32, 66, 8192], P('exp', None, None, 'seq'), may hold values from -6 to 6
- w_down: bfloat16 [4, 8192, 2048], P('exp', 'seq'), may hold values from -0.0029296875 to 0.0029296875
Outputs:
- d_inner: bfloat16 [4096, 4096], P('seq', 'exp')
- d_gate: float32 [2, 4096], P(None, ('seq', 'exp'))
The draws below stay inside these ranges and needn't reach their ends.
Inputs may be any that keep to these rules, and one draw needn't show every extreme that they name: `expert_ids`: each row names 2 different experts. Within the rows of one token group no expert is named by more than 66 rows, and in every draw some expert is named by exactly 66 rows of some group. `log_decay`: every entry is negative.
All inputs are finite; a program needn't handle non-finite values.
Results may differ from the reference program's by a relative error of at most 0.00065.
Values may be sent and summed in bfloat16 or wider, within the bound.
No kernel may reach another device: no remote copies, remote signals or barrier semaphores. Data moves between devices by JAX's collectives and lax.ppermute only.
A program may use at most 128 MiB of HBM per device.

```python
import math
from functools import partial
import jax
import jax.numpy as jnp
import numpy as np
from jax import lax

D = 2048
INNER = 4096
STATE = 16
HEAD = 64
FF = 8192
TOP = 2
TOK_DEV = 128
EXPERTS = 4
CAP = 66
SEQ_ROWS = 512
SEQUENCE_ITEMS = 4096
SOURCES = 32
HEADS = 64


def draw_log_decay(key, part):
    stochastic_seeds = jax.random.split(key, 7)
    slow_rate = jnp.exp(jax.random.uniform(stochastic_seeds[0], (HEADS, 1), jnp.float32, math.log(0.1 / SEQUENCE_ITEMS), math.log(0.8 / SEQUENCE_ITEMS)))
    fast_rate = jnp.exp(jax.random.uniform(stochastic_seeds[1], (HEADS, 1), jnp.float32, math.log(0.02), math.log(0.05)))
    slow_mask = jax.random.bernoulli(stochastic_seeds[2], 0.5, (HEADS, 1))
    per_channel_forgetting = jnp.where(slow_mask, slow_rate, fast_rate)
    forgetting_noise = jnp.exp(jax.random.uniform(stochastic_seeds[3], (HEADS, SEQUENCE_ITEMS), jnp.float32, math.log(0.5), math.log(2.0)))
    shard_draw = jnp.exp(jax.random.uniform(stochastic_seeds[4], (HEADS, SEQUENCE_ITEMS // SEQ_ROWS), jnp.float32, math.log(0.5), math.log(2.0)))
    shard_multiplier = jnp.repeat(shard_draw, SEQ_ROWS, axis=1)
    spike_opening_slot = jax.random.randint(stochastic_seeds[5], (2, 1), 0, SEQUENCE_ITEMS)
    spike_span = jax.random.uniform(stochastic_seeds[6], (2, 1), jnp.float32, 0.22, 0.45)
    sequence_offsets = lax.broadcasted_iota(jnp.int32, (2, SEQUENCE_ITEMS), 1)
    spike_table = jnp.sum(jnp.where(sequence_offsets == spike_opening_slot, spike_span, 0.0), axis=0)
    return -(per_channel_forgetting * forgetting_noise * shard_multiplier) - spike_table[None, :]


def level_of(rng, dims, shards, low, largest):
    gain = 1.0
    for dim, parts in shards:
        steps = jax.random.uniform(jax.random.fold_in(jax.random.fold_in(rng, 6), dim), (parts,), jnp.float32, low / len(shards), largest / len(shards))
        gain = gain * jnp.repeat(jnp.exp(steps), dims[dim] // parts).reshape((-1,) + (1,) * (len(dims) - 1 - dim))
    return gain


def assign_block(key, own, number, rows, amount, top, limit, skew):
    ranking = jax.random.permutation(key, amount)
    heavy_load, usual = shares(amount, rows * top, limit, skew, True), shares(amount, rows * top, limit, skew, False)
    places = jnp.arange(amount)

    def named(lengths, turn):
        used = int((lengths > 0).sum())
        fixed = max(1, used // 4)
        passed = fixed + (places - fixed + turn * (used - fixed)) % max(1, amount - fixed)
        return jnp.zeros((amount,), jnp.int32).at[ranking[jnp.where(places < fixed, places, passed)]].set(jnp.asarray(lengths, jnp.int32))

    lengths = jnp.where(number % 4 == 0, named(heavy_load, number // 4), named(usual, number - number // 4 - 1))
    mixed = jax.random.permutation(jax.random.fold_in(own, 3), amount)
    giver, taker = mixed[0:amount // 2 * 2:2], mixed[1:amount // 2 * 2:2]
    room = jnp.minimum(lengths[giver] - 1, limit - lengths[taker]) // 2
    room = jnp.where((giver == ranking[0]) | (taker == ranking[0]) | (lengths[taker] == 0), 0, jnp.maximum(room, 0))
    passed = jax.random.randint(jax.random.fold_in(own, 4), (amount // 2,), 0, 1 << 20) % (room + 1)
    lengths = lengths.at[giver].add(-passed).at[taker].add(passed)
    members = jnp.searchsorted(jnp.cumsum(lengths), jnp.arange(rows * top), side="right").astype(jnp.int32)
    table = members.reshape(top, rows).T
    table = table[jax.random.permutation(jax.random.fold_in(own, 1), rows)]
    turn = jax.random.randint(jax.random.fold_in(own, 2), (rows, 1), 0, top)
    return jnp.take_along_axis(table, (jnp.arange(top)[None, :] + turn) % top, axis=1)


def shares(amount, total, limit, slope, full):
    portions = [(1 << 20) // math.isqrt(standing ** slope) + 1 for standing in range(1, amount + 1)]
    largest = limit if full else min(limit, max(-(-total // amount), total * portions[0] // sum(portions)))
    least = 1 if total - largest >= amount - 1 else 0
    given, spare = [largest] + [least] * (amount - 1), total - largest - least * (amount - 1)
    while spare > 0:
        free = [i for i in range(1, amount) if given[i] < largest] or [i for i in range(1, amount) if given[i] < limit]
        mass, remaining = sum([portions[i] for i in free]), spare
        for i in free:
            more = min(limit - given[i], max(1, remaining * portions[i] // mass), spare)
            given[i] = given[i] + more
            spare = spare - more
    return np.array(given)


def normal_values(key, dims, width, bound, cuts=(), kind=jnp.bfloat16):
    entries = width * jax.random.normal(key, dims, jnp.float32)
    if cuts:
        entries = entries * level_of(key, dims, cuts, -0.22, 0.18)
    return jnp.clip(entries, -bound, bound).astype(kind)


def setup_inputs(seed: int = 0) -> dict:
    streams_of = jax.random.split(jax.random.key(seed), 11)
    grad_out = normal_values(streams_of[0], (SEQUENCE_ITEMS, D), 1.0, 6.0, ((0, 32),))
    out_proj = normal_values(streams_of[1], (INNER, D), D ** -0.5, 0.125, ((0, 4),))
    step_size = jnp.clip(jnp.exp(math.log(0.1) - 4.6051702 * jax.random.uniform(streams_of[2], (HEADS, SEQUENCE_ITEMS), jnp.float32) ** level_of(streams_of[2], (HEADS, SEQUENCE_ITEMS), ((0, 4), (1, 8)), -0.2, 0.2)), 0.001, 0.1)
    log_decay = draw_log_decay(jax.random.fold_in(streams_of[10], 71), 0)
    b_input = normal_values(streams_of[4], (STATE, SEQUENCE_ITEMS), 0.25, 1.5, ((1, 8),), jnp.float32)
    c_output = normal_values(streams_of[5], (STATE, SEQUENCE_ITEMS), 0.25, 1.5, ((1, 8),), jnp.float32)
    skip_gain = jnp.clip(0.5 + 1.0 * jax.random.uniform(streams_of[6], (INNER,), jnp.float32) ** level_of(streams_of[6], (INNER,), ((0, 4),), -0.2, 0.2), 0.5, 1.5)
    expert_ids_keys = jax.random.split(jax.random.fold_in(streams_of[7], 1), SEQUENCE_ITEMS // TOK_DEV)
    expert_ids_turns = jax.random.permutation(jax.random.fold_in(streams_of[7], 3), SEQUENCE_ITEMS // TOK_DEV)
    expert_ids = jax.vmap(lambda own, number: assign_block(jax.random.fold_in(streams_of[7], 2), own, number, TOK_DEV, EXPERTS, TOP, CAP, 0))(expert_ids_keys, expert_ids_turns).reshape((SEQUENCE_ITEMS, TOP))
    hidden_act = normal_values(streams_of[8], (EXPERTS, SOURCES, CAP, FF), 1.0, 6.0, ((0, 4), (3, 8)))
    w_down = normal_values(streams_of[9], (EXPERTS, FF, D), (FF * D // 4) ** -0.5, 0.0029296875, ((0, 4), (1, 8)))
    return {"grad_out": grad_out, "out_proj": out_proj, "step_size": step_size, "log_decay": log_decay, "b_input": b_input, "c_output": c_output, "skip_gain": skip_gain, "expert_ids": expert_ids, "hidden_act": hidden_act, "w_down": w_down}


highest = lax.Precision.HIGHEST


def block_pass(state_in, pieces):
    grad_block, decay_block, step_block, b_block, c_block = pieces
    cum_decay = jnp.cumsum(decay_block, axis=1)
    gap_table = cum_decay[:, None, :] - cum_decay[:, :, None]
    upper_mask = lax.broadcasted_iota(jnp.int32, gap_table.shape, 2) >= lax.broadcasted_iota(jnp.int32, gap_table.shape, 1)
    weights = jnp.where(upper_mask, jnp.exp(jnp.where(upper_mask, gap_table, 0.0)), 0.0)
    intersection = lax.dot_general(b_block, c_block, (((0,), (0,)), ((), ())), precision=highest, preferred_element_type=jnp.float32)
    within = jnp.einsum("hut,thp->uhp", weights * intersection[None], grad_block, precision=highest)
    tail_decay = jnp.exp(cum_decay[:, -1:] - cum_decay)
    from_state = jnp.einsum("nu,hnp->uhp", b_block, state_in, precision=highest) * tail_decay.T[:, :, None]
    result = step_block.T[:, :, None] * (within + from_state)
    state_out = jnp.einsum("ht,nt,thp->hnp", jnp.exp(cum_decay), c_block, grad_block, precision=highest)
    state_out = state_out + jnp.exp(cum_decay[:, -1])[:, None, None] * state_in
    return state_out, result


def local_sweep(grad_rows, decay_rows, step_rows, b_rows, c_rows, start_state):
    row_count = grad_rows.shape[0]
    head_count = decay_rows.shape[0]
    block_len = min(512, row_count)
    block_count = row_count // block_len
    pieces = (grad_rows.reshape(block_count, block_len, head_count, grad_rows.shape[2]),
              decay_rows.reshape(head_count, block_count, block_len).transpose(1, 0, 2),
              step_rows.reshape(head_count, block_count, block_len).transpose(1, 0, 2),
              b_rows.reshape(b_rows.shape[0], block_count, block_len).transpose(1, 0, 2),
              c_rows.reshape(c_rows.shape[0], block_count, block_len).transpose(1, 0, 2))
    state_out, results = lax.scan(block_pass, start_state, pieces, reverse=True)
    return state_out, results.reshape(row_count, head_count, grad_rows.shape[2])


def route_table(groups, expert, cap_len):
    hit_mask = jnp.any(groups == expert, axis=2)
    rank_ids = jnp.cumsum(hit_mask.astype(jnp.int32), axis=1) - 1
    slot_ids = lax.broadcasted_iota(jnp.int32, (1, 1, cap_len), 2)
    chosen = jnp.logical_and(hit_mask[:, :, None], rank_ids[:, :, None] == slot_ids)
    token_ids = lax.broadcasted_iota(jnp.int32, chosen.shape, 1)
    position = jnp.sum(jnp.where(chosen, token_ids, 0), axis=1).astype(jnp.int32)
    filled = jnp.any(chosen, axis=1)
    return position, filled


def slot_lookup(slot_table, own_ids, cap_len, expert_count):
    experts_iota = lax.broadcasted_iota(jnp.int32, (1, 1, expert_count), 2)
    onehot = own_ids[:, :, None] == experts_iota
    member = jnp.any(onehot, axis=1).astype(jnp.int32)
    rank_ids = jnp.cumsum(member, axis=0) - 1
    slot_of = jnp.sum(jnp.where(onehot, rank_ids[:, None, :], 0), axis=2)
    picked = jnp.sum(jnp.where(onehot[:, :, :, None], slot_table[None, None], 0.0), axis=2)
    slot_iota = lax.broadcasted_iota(jnp.int32, (1, 1, cap_len), 2)
    return jnp.sum(jnp.where(slot_of[:, :, None] == slot_iota, picked, 0.0), axis=2)


def reference(grad_out, out_proj, step_size, log_decay, b_input, c_output, skip_gain, expert_ids, hidden_act, w_down):
    inner_grad = jnp.dot(grad_out, out_proj.T, preferred_element_type=jnp.float32)
    start_state = jnp.zeros((HEADS, STATE, HEAD), jnp.float32)
    unused, swept_part = local_sweep(inner_grad.reshape(SEQUENCE_ITEMS, HEADS, HEAD), log_decay, step_size, b_input, c_output, start_state)
    d_inner = (swept_part.reshape(SEQUENCE_ITEMS, INNER) + skip_gain * inner_grad).astype(jnp.bfloat16)
    groups = expert_ids.reshape(SOURCES, TOK_DEV, TOP)
    sources = grad_out.reshape(SOURCES, TOK_DEV, D)

    def per_expert(pieces):
        expert, saved_part, weights = pieces
        position, filled = route_table(groups, expert, CAP)
        slot_rows = jnp.take_along_axis(sources, position[:, :, None], axis=1)
        slot_rows = jnp.where(filled[:, :, None], slot_rows, jnp.zeros_like(slot_rows))
        projected = jnp.dot(slot_rows.reshape(SOURCES * CAP, D), weights.T, preferred_element_type=jnp.float32)
        scores = jnp.sum(projected * saved_part.reshape(SOURCES * CAP, FF).astype(jnp.float32), axis=1)
        return scores.reshape(SOURCES, CAP)

    slot_scores = lax.map(per_expert, (jnp.arange(EXPERTS, dtype=jnp.int32), hidden_act, w_down))
    lookup = partial(slot_lookup, cap_len=CAP, expert_count=EXPERTS)
    values = jax.vmap(lookup, in_axes=(1, 0))(slot_scores, groups)
    d_gate = values.reshape(SEQUENCE_ITEMS, TOP).T
    return d_inner, d_gate
```

```python
import functools

import jax
import jax.numpy as jnp
from jax import lax
from jax.experimental import pallas as pl
from jax.experimental.pallas import tpu as pltpu
from jax.sharding import PartitionSpec as P

HEAD = 64
LANES = 128
SLOT_ROWS = 16
F32 = jnp.float32
BF16 = jnp.bfloat16
HIGHEST = lax.Precision.HIGHEST
NN = (((1,), (0,)), ((), ()))
NT = (((1,), (1,)), ((), ()))
TN = (((0,), (0,)), ((), ()))
MIB = 2**20


def dot(a, b, dims=NN, precision=None):
    return lax.dot_general(a, b, dims, precision=precision, preferred_element_type=F32)


def split(value):
    high = value.astype(BF16)
    return high, (value - high.astype(F32)).astype(BF16)


def iota(shape, dim):
    return lax.broadcasted_iota(jnp.int32, shape, dim)


def call(body, name, ins, outs, scratch=(), after=(), flops=10**8, limit=8 * MIB):
    vmem = pl.BlockSpec(memory_space=pltpu.VMEM)
    wait = pl.BlockSpec(memory_space=pl.ANY)
    skip = len(after)

    def kernel(*refs):
        body(*refs[skip:])

    return pl.pallas_call(
        kernel,
        name=name,
        out_shape=tuple(outs),
        in_specs=[wait] * skip + [vmem] * len(ins),
        out_specs=tuple([vmem] * len(outs)),
        scratch_shapes=list(scratch),
        compiler_params=pltpu.CompilerParams(vmem_limit_bytes=limit),
        cost_estimate=pl.CostEstimate(flops=flops, bytes_accessed=flops // 100, transcendentals=0),
    )(*after, *ins)


def shape(dims, dtype=F32):
    return jax.ShapeDtypeStruct(dims, dtype)


def ring_index(k):
    count = lax.axis_size("exp")
    return lax.rem(lax.axis_index("exp") + count - k, count)


def part_of(index, size):
    return pl.ds(pl.multiple_of(index * size, size), size)


def slot_match(ids, expert, slots):
    tokens = ids.shape[1]
    hit = jnp.max((ids == expert).astype(F32), axis=0, keepdims=True)
    upper = (iota((tokens, tokens), 0) <= iota((tokens, tokens), 1)).astype(BF16)
    rank = dot(jnp.broadcast_to(hit, (8, tokens)).astype(BF16), upper)[0:1]
    rank = jnp.where(hit > 0.0, rank - 1.0, -1.0)
    return iota((slots, tokens), 0).astype(F32) == rank


def pick_rows(match, pieces, out_ref):
    cap = out_ref.shape[0]
    start = 0
    for piece in pieces:
        width = piece.shape[1]
        out_ref[:, start:start + width] = dot(match, piece[...]).astype(BF16)[:cap]
        start += width


def route_body(count, blocks, *refs):
    ids_ref, pieces, match_ref, out_ref = refs[0], refs[1:1 + count], refs[-2], refs[-1]
    tokens = pieces[0].shape[0]
    for k in range(blocks):
        ids = ids_ref[:, part_of(ring_index(k), tokens)]
        match_ref[k] = slot_match(ids, lax.axis_index("exp"), match_ref.shape[1]).astype(BF16)
    pick_rows(match_ref[0], pieces, out_ref)


def select_body(count, k, *refs):
    pick_rows(refs[0][k], refs[1:1 + count], refs[-1])


def choose_body(first_ref, second_ref, out_ref):
    even = lax.rem(lax.axis_index("seq"), 2) == 0

    @pl.when(even)
    def _():
        out_ref[...] = first_ref[...]

    @pl.when(jnp.logical_not(even))
    def _():
        out_ref[...] = second_ref[...]


def own_groups_body(groups, cap, saved_ref, out_ref):
    exp_count = lax.axis_size("exp")
    core = lax.rem(lax.axis_index("seq"), 2)
    kept = out_ref.shape[0]
    rows, cols = kept * SLOT_ROWS, groups * SLOT_ROWS
    row, col = iota((rows, cols), 0), iota((rows, cols), 1)
    item = row // SLOT_ROWS
    group = (item // exp_count * 2 + core) * exp_count + item % exp_count
    pick = ((row % SLOT_ROWS == col // groups) & (col % groups == group)).astype(BF16)
    for start in range(0, cap, SLOT_ROWS):
        depth = min(SLOT_ROWS, cap - start) * groups
        for left in range(0, out_ref.shape[2], 512):
            lanes = slice(left, min(left + 512, out_ref.shape[2]))
            block = saved_ref[start * groups:start * groups + depth, lanes]
            value = dot(pick[:, :depth], block).astype(BF16)
            for i in range(kept):
                out_ref[i, start:start + SLOT_ROWS, lanes] = value[i * SLOT_ROWS:(i + 1) * SLOT_ROWS]


def own_groups(hidden_act, chips, exp_count, after=()):
    groups, cap, hidden = hidden_act.shape[1:]
    pad = -(-cap // SLOT_ROWS) * SLOT_ROWS
    kept = chips * exp_count
    if groups * SLOT_ROWS <= 1024:
        saved = jnp.transpose(hidden_act[0], (1, 0, 2)).reshape(cap * groups, hidden)
        return call(functools.partial(own_groups_body, groups, cap), "own_groups", [saved],
                    [shape((kept, pad, hidden), BF16)], after=after, flops=10**9,
                    limit=24 * MIB)[0]
    core = lax.rem(lax.axis_index("seq"), 2)
    saved = hidden_act.reshape(chips, 2, exp_count, cap, hidden)
    saved = lax.dynamic_index_in_dim(saved, core, 1, False).reshape(kept, cap, hidden)
    return jnp.pad(saved, ((0, 0), (0, pad - cap), (0, 0)))


def score_body(masks, k, rows, own_h, other_h, own_w, other_w, out_ref, packed, total):
    exp_count = lax.axis_size("exp")
    pad = own_h.shape[1]
    cap = rows[0].shape[0]
    tile = 256
    chip = lax.axis_index("seq") // 2
    for m in range(len(masks)):
        packed[(m + 1) * pad - SLOT_ROWS:(m + 1) * pad, :] = jnp.zeros(
            (SLOT_ROWS, packed.shape[1]), BF16)
        packed[m * pad:m * pad + cap, :] = rows[m][...]
    total[...] = jnp.zeros_like(total)
    items = [lax.bitwise_xor(chip, mask) * exp_count + ring_index(k) for mask in masks]

    def step(i, carry):
        cols = part_of(i, tile)
        for weight, saved in ((own_w, own_h), (other_w, other_h)):
            projected = dot(packed[...], weight[cols, :], NT)
            for m, item in enumerate(items):
                product = projected[m * pad:(m + 1) * pad] * saved[item, :, cols].astype(F32)
                folded = product[:, 0:LANES]
                for j in range(1, tile // LANES):
                    folded = folded + product[:, j * LANES:(j + 1) * LANES]
                total[m * pad:(m + 1) * pad, :] += folded
        return carry

    lax.fori_loop(0, own_w.shape[0] // tile, step, 0)
    out_ref[...] = jnp.zeros_like(out_ref)
    ones = jnp.ones((8, LANES), F32)
    for m in range(len(masks)):
        out_ref[m:m + 1, 0:pad] = dot(ones, total[m * pad:(m + 1) * pad], NT, HIGHEST)[0:1]


def score(masks, k, rows, own_h, other_h, own_w, other_w, after):
    count = len(masks)
    pad, width = own_h.shape[1], own_w.shape[1]

    def body(*refs):
        score_body(masks, k, refs[:count], *refs[count:])

    return call(body, "score", [*rows, own_h, other_h, own_w, other_w],
                [shape((count, LANES))],
                [pltpu.VMEM((count * pad, width), BF16), pltpu.VMEM((count * pad, LANES), F32)],
                after, flops=4 * 10**9, limit=6 * MIB)[0]


def decay_sums(log_decay):
    length = log_decay.shape[1]
    upper = (iota((length, length), 0) <= iota((length, length), 1)).astype(F32)
    return dot(log_decay, upper, NN, HIGHEST)


def mixer_block_body(count, k, *refs):
    pieces = refs[:count]
    proj_ref, step_ref, decay_ref, b_ref, c_ref, skip_ref = refs[count:count + 6]
    acc_ref, sum_ref, grad_ref = refs[count + 6:]
    tokens = pieces[0].shape[0]
    heads, states = step_ref.shape[0], b_ref.shape[0]
    start, total = 0, None
    for piece in pieces:
        width = piece.shape[1]
        term = dot(piece[...], proj_ref[:, start:start + width], NT)
        total = term if total is None else total + term
        start += width
    grad_ref[...] = total
    here = part_of(ring_index(k), tokens)
    cum = decay_sums(decay_ref[:, here])
    cum_t = cum.T
    step_t = step_ref[:, here].T
    c_here = c_ref[:, here]
    keep = iota((tokens, tokens), 1) >= iota((tokens, tokens), 0)
    inter = jnp.where(keep, dot(b_ref[:, here], c_here, TN, HIGHEST), 0.0)
    lane = iota((tokens, LANES), 1)
    grow = jnp.exp(cum)
    per = LANES // HEAD
    for pair in range(heads // per):
        cols = slice(pair * LANES, (pair + 1) * LANES)
        grad = grad_ref[:, cols]
        g_high, g_low = split(grad)
        lefts = []
        for head in range(pair * per, (pair + 1) * per):
            gap = jnp.where(keep, cum[head:head + 1, :] - cum_t[:, head:head + 1], 0.0)
            lefts.append(jnp.exp(gap) * inter * step_t[:, head:head + 1])
        for head in range(pair * per, (pair + 1) * per):
            lefts.append(c_here * grow[head:head + 1, :])
        l_high, l_low = split(jnp.concatenate(lefts, axis=0))
        out = dot(l_high, g_high) + (dot(l_low, g_high) + dot(l_high, g_low))
        within = out[0:tokens]
        base = per * tokens
        state = out[base:base + states]
        for i in range(1, per):
            within = jnp.where(lane >= i * HEAD, out[i * tokens:(i + 1) * tokens], within)
            state = jnp.where(lane[:states] >= i * HEAD,
                              out[base + i * states:base + (i + 1) * states], state)
        acc_ref[:, cols] = within + skip_ref[0:1, cols] * grad
        sum_ref[:, cols] = state


def spread(values, lane):
    out = values[:, 0:1]
    for i in range(1, LANES // HEAD):
        out = jnp.where(lane >= i * HEAD, values[:, i:i + 1], out)
    return jnp.broadcast_to(out, lane.shape)


def shard_sum_body(count, decay_ref, *refs):
    sums, out_ref, hold = refs[:count], refs[count], refs[count + 1]
    states, chans = sums[0].shape
    tokens = decay_ref.shape[1] // count
    per = LANES // HEAD
    for k in range(count):
        hold[ring_index(k)] = sums[k][...]
    totals = [jnp.sum(decay_ref[:, j * tokens:(j + 1) * tokens], axis=1, keepdims=True).T
              for j in range(count)]
    lane = iota((1, LANES), 1)
    for pair in range(chans // LANES):
        cols = slice(pair * LANES, (pair + 1) * LANES)
        state = jnp.zeros((states, LANES), F32)
        total = jnp.zeros((1, LANES), F32)
        for j in reversed(range(count)):
            here = spread(totals[j][:, pair * per:(pair + 1) * per], lane)
            state = hold[j, :, cols] + jnp.exp(here) * state
            total = total + here
        out_ref[0:states, cols] = state
        out_ref[states:, cols] = jnp.broadcast_to(total, (8, LANES))


def joined(bit, group, got, carried):
    states = group.shape[0] - 8
    earlier = (lax.axis_index("seq") & bit) == 0
    theirs, decay = got[:states], got[states:]
    if carried is None:
        inside, after = jnp.zeros_like(theirs), jnp.zeros_like(decay)
    else:
        inside, after = carried[:states], carried[states:]
    inside = inside + jnp.where(earlier, jnp.exp(after[0:1]) * theirs, 0.0)
    after = after + jnp.where(earlier, decay, 0.0)
    return earlier, inside, after


def combine_body(bit, *refs):
    group_ref, got_ref, carry = refs[0], refs[1], refs[2:-2]
    new_ref, out_ref = refs[-2:]
    group, got = group_ref[...], got_ref[...]
    earlier, inside, after = joined(bit, group, got, carry[0][...] if carry else None)
    states = inside.shape[0]
    out_ref[0:states, :] = inside
    out_ref[states:, :] = after
    front, back = jnp.where(earlier, group, got), jnp.where(earlier, got, group)
    new_ref[0:states, :] = front[:states] + jnp.exp(front[states:states + 1]) * back[:states]
    new_ref[states:, :] = group[states:] + got[states:]


def final_body(bit, count, *refs):
    group_ref, got_ref, carry_ref, step_ref, decay_ref, b_ref = refs[:6]
    sums, accs = refs[6:6 + count], refs[6 + count:6 + 2 * count]
    out_ref, hold, scale_ref, left_ref = refs[6 + 2 * count:]
    tokens = decay_ref.shape[1] // count
    chans = out_ref.shape[1]
    per = LANES // HEAD
    carried = carry_ref[...] if carry_ref.shape[0] == group_ref.shape[0] else None
    incoming = joined(bit, group_ref[...], got_ref[...], carried)[1]
    totals = []
    for k in range(count):
        hold[ring_index(k)] = sums[k][...]
    for j in range(count):
        part = slice(j * tokens, (j + 1) * tokens)
        cum = decay_sums(decay_ref[:, part])
        total = cum[:, tokens - 1:tokens]
        scale_ref[j] = (step_ref[:, part] * jnp.exp(total - cum)).T
        left_ref[j] = b_ref[:, part].T
        totals.append(total.T)
    lane = iota((tokens, LANES), 1)
    for pair in range(chans // LANES):
        cols = slice(pair * LANES, (pair + 1) * LANES)
        heads = slice(pair * per, (pair + 1) * per)
        state = incoming[:, cols]
        for j in reversed(range(count)):
            mine = hold[j, :, cols]
            hold[j, :, cols] = state
            state = mine + jnp.exp(spread(totals[j][:, heads], lane[0:1])) * state
    for k in range(count):
        j = ring_index(k)
        l_high, l_low = split(left_ref[j])
        scale = scale_ref[j]
        rows = part_of(j, tokens)
        s_high, s_low = split(hold[j])
        term = dot(l_high, s_high) + (dot(l_low, s_high) + dot(l_high, s_low))
        for pair in range(chans // LANES):
            cols = slice(pair * LANES, (pair + 1) * LANES)
            heads = slice(pair * per, (pair + 1) * per)
            value = accs[k][:, cols] + term[:, cols] * spread(scale[:, heads], lane)
            out_ref[rows, cols] = value.astype(BF16)


def gate_body(count, ids_ref, *refs):
    tables, out_ref = refs[:-1], refs[-1]
    tokens = out_ref.shape[1]
    own = lax.axis_index("exp")
    ids = ids_ref[:, part_of(own, tokens)]
    result = jnp.zeros(out_ref.shape, F32)
    for k in range(count):
        expert = lax.rem(own + k, count)
        match = slot_match(ids, expert, LANES).astype(F32)
        table = jnp.broadcast_to(tables[k][...], (8, LANES))
        value = dot(table, match, NN, HIGHEST)[0:1]
        result = result + jnp.where(ids == expert, value, 0.0)
    out_ref[...] = result


def shards(grad_out, out_proj, step_size, log_decay, b_input, c_output, skip_gain, expert_ids,
           hidden_act, w_down):
    exp_count, seq_count = lax.axis_size("exp"), lax.axis_size("seq")
    tokens, width = grad_out.shape
    cap, hidden = hidden_act.shape[2:]
    chips = seq_count // 2
    heads, states, chans = step_size.shape[0], b_input.shape[0], out_proj.shape[0]
    pad = -(-cap // SLOT_ROWS) * SLOT_ROWS
    halves = 1

    def across(value, flip):
        return lax.ppermute(value, "seq", [(s, s ^ flip(s)) for s in range(seq_count)])

    other_w = across(w_down[0], lambda s: 1)
    other_h = across(hidden_act, lambda s: 1)
    ids = expert_ids.T
    skip = skip_gain.reshape(1, -1)
    cut = width // halves
    pieces = [grad_out[:, i * cut:(i + 1) * cut] for i in range(halves)]
    matches, slots = call(
        functools.partial(route_body, halves, exp_count), "route", [ids, *pieces],
        [shape((exp_count, pad, tokens), BF16), shape((cap, width), BF16)])

    def spread_slots(value):
        held = {0: value}
        for mask in sorted(range(1, chips), key=lambda m: (bin(m).count("1"), m)):
            low, high = mask & -mask, 1 << (mask.bit_length() - 1)
            if low != high:
                value = call(choose_body, "choose", [held[mask ^ high], held[mask ^ low]],
                             [shape((cap, width), BF16)])[0]
            held[mask] = across(value, lambda s: 2 * (high if s % 2 == 0 else low))
        return held

    accs, sums, helds = [], [], []
    own_h = own_groups(hidden_act, chips, exp_count, (slots,))
    saved_h = None
    found = []

    def score_block(k, masks, after):
        return score(masks, k, [helds[k][m] for m in masks], own_h, saved_h, w_down[0], other_w,
                     after)

    all_masks = list(range(chips))
    for k in range(exp_count):
        if k:
            ring = [(e, (e + 1) % exp_count) for e in range(exp_count)]
            pieces = [lax.ppermute(piece, "exp", ring) for piece in pieces]
            slots = call(functools.partial(select_body, halves, k), "select",
                         [matches, *pieces], [shape((cap, width), BF16)], after=last)[0]
        helds.append(spread_slots(slots))
        acc, total = call(
            functools.partial(mixer_block_body, halves, k), "mixer_block",
            [*pieces, out_proj, step_size, log_decay, b_input, c_output, skip],
            [shape((tokens, chans)), shape((states, chans))],
            [pltpu.VMEM((tokens, chans), F32)], after=(slots,), flops=10**9)
        accs.append(acc)
        sums.append(total)
        last = (total,)
        if k == 1:
            saved_h = own_groups(other_h, chips, exp_count, (total,))
        if k >= 1 and k < exp_count - 1 or (k == 1):
            found.append(score_block(len(found), all_masks, last))
            last = (found[-1],)

    summary = call(functools.partial(shard_sum_body, exp_count), "shard_sum", [log_decay, *sums],
                   [shape((states + 8, chans))],
                   [pltpu.VMEM((exp_count, states, chans), F32)])[0]
    while len(found) < exp_count - 1:
        found.append(score_block(len(found), all_masks, (summary, found[-1])))
    group, carried, bit = summary, step_size, 1
    while True:
        got = across(group, lambda s: bit)
        if 2 * bit >= seq_count:
            break
        carry = [] if bit == 1 else [carried]
        group, carried = call(functools.partial(combine_body, bit), "combine",
                              [group, got, *carry], [shape((states + 8, chans))] * 2)
        bit *= 2
    first = [m for m in all_masks if bin(m).count("1") <= 1]
    rest = [m for m in all_masks if m not in first]
    last_k = exp_count - 1
    tail = {}
    if exp_count > 1:
        masks_of = [first, rest] if rest else [first]
    for masks in masks_of:
        out = score_block(last_k, masks, (found[-1],))
        for i, m in enumerate(masks):
            tail[m] = out[i:i + 1]

    d_inner = call(
        functools.partial(final_body, bit, exp_count), "mixer_final",
        [group, got, carried, step_size, log_decay, b_input, *sums, *accs],
        [shape((exp_count * tokens, chans), BF16)],
        [pltpu.VMEM((exp_count, states, chans), F32),
         pltpu.VMEM((exp_count, tokens, heads), F32),
         pltpu.VMEM((exp_count, tokens, states), F32)], flops=10**9)[0]

    def scores_of(m):
        return jnp.concatenate([f[m:m + 1] for f in found] + [tail[m]], axis=0)

    summed = scores_of(0)
    for m in range(1, chips):
        summed = summed + across(scores_of(m), lambda s: 2 * m)
    tables = []
    for k in range(exp_count):
        table = summed[k:k + 1]
        if k:
            table = lax.ppermute(table, "exp",
                                 [(e, (e - k) % exp_count) for e in range(exp_count)])
        tables.append(table)
    d_gate = call(functools.partial(gate_body, exp_count), "gate", [ids, *tables],
                  [shape((expert_ids.shape[1], tokens))])[0]
    return d_inner, d_gate


def solution(mesh):
    in_specs = (
        P(("seq", "exp"), None),
        P("exp", None),
        P("exp", "seq"),
        P("exp", "seq"),
        P(None, "seq"),
        P(None, "seq"),
        P("exp"),
        P("seq", None),
        P("exp", None, None, "seq"),
        P("exp", "seq", None),
    )
    out_specs = (P("seq", "exp"), P(None, ("seq", "exp")))
    return jax.shard_map(shards, mesh=mesh, in_specs=in_specs, out_specs=out_specs, check_vma=False)
```
